32 devices in a mesh: rep: 2 (over x), dp: 16 (over y, z, core).
Axes of the slice: x: 2, y: 2, z: 4, core: 2. Of those that a mesh axis runs over, the one named last changes fastest.
Arguments:
- x: bfloat16 [32, 2048, 1024], P(('rep', 'dp')), parts along dimension 0
- dy: bfloat16 [32, 2048, 1024], P(('rep', 'dp')), parts along dimension 0
- w_gate: bfloat16 [2, 1024, 3200], replicated
- w_up: bfloat16 [2, 1024, 3200], replicated
- w_down: bfloat16 [2, 3200, 1024], replicated
- m_w_gate: float32 [2, 1024, 3200], replicated
- m_w_up: float32 [2, 1024, 3200], replicated
- m_w_down: float32 [2, 3200, 1024], replicated
- v_w_gate: float32 [2, 1024, 3200], replicated
- v_w_up: float32 [2, 1024, 3200], replicated
- v_w_down: float32 [2, 3200, 1024], replicated
Outputs:
- output 1: bfloat16 [4, 1024, 3200], P('rep'), parts along dimension 0
- output 2: bfloat16 [4, 1024, 3200], P('rep'), parts along dimension 0
- output 3: bfloat16 [4, 3200, 1024], P('rep'), parts along dimension 0
- output 4: float32 [4, 1024, 3200], P('rep'), parts along dimension 0
- output 5: float32 [4, 1024, 3200], P('rep'), parts along dimension 0
- output 6: float32 [4, 3200, 1024], P('rep'), parts along dimension 0
- output 7: float32 [4, 1024, 3200], P('rep'), parts along dimension 0
- output 8: float32 [4, 1024, 3200], P('rep'), parts along dimension 0
- output 9: float32 [4, 3200, 1024], P('rep'), parts along dimension 0
There are 2 independent parts. The reference program is written for one: setup_inputs(seed, part) draws one part's arguments, and reference() takes and returns one part's arrays. A program takes and returns all parts, laid end to end along the dimension named above; an argument that names none is the same for every part.
All inputs are finite; a program needn't handle non-finite values.
Results may differ from the reference program's by a relative error of at most 0.022.
Values are sent between devices in bfloat16 or wider.
A program may use at most 2.75 GiB of HBM per device.

```python
import jax
import jax.numpy as jnp
from jax import lax

SEQUENCES = 16
TOKENS = 2048
D = 1024
FF = 3200
LAYERS = 2
NAMES = ("w_gate", "w_up", "w_down")
SHAPES = {"w_gate": (LAYERS, D, FF), "w_up": (LAYERS, D, FF), "w_down": (LAYERS, FF, D)}


def bump(key, n, height):
    away = (jnp.arange(n, dtype=jnp.int32) - jax.random.randint(key, (), 0, n, jnp.int32)) % n
    return jnp.where(away < n // 8, height, 1.0)


def together(key, own, strength):
    shared = jax.random.normal(key, own.shape[1:], jnp.float32)
    return (own + strength * shared) * lax.rsqrt(1 + strength * strength)


def setup_inputs(seed: int = 0, part: int = 0) -> dict:
    kx, kdy, ka, kb, kz, kf, kh, kl, *keys = jax.random.split(jax.random.key(seed), 8 + 3 * len(NAMES))
    kx, kdy, ka, kb = (jax.random.fold_in(k, part) for k in (kx, kdy, ka, kb))
    kw, km, kv = (keys[i::3] for i in range(3))
    shape = (SEQUENCES, TOKENS, D)
    much_x, much_dy = jax.random.uniform(kz, (2,), jnp.float32, 0.0, 1.0)
    loud = 2.0 ** jax.random.uniform(jax.random.fold_in(kz, 1), (), jnp.float32, -1.0, 2.0)
    layers = 2.0 ** jax.random.uniform(kl, (LAYERS, 1, 1), jnp.float32, -1.0, 1.0)
    x = together(ka, jax.random.normal(kx, shape, jnp.float32), much_x) * bump(kf, D, 4.0)
    dy = together(kb, jax.random.normal(kdy, shape, jnp.float32), much_dy)
    drawn = {"x": x.astype(jnp.bfloat16), "dy": (loud * dy * (SEQUENCES * TOKENS) ** -0.5).astype(jnp.bfloat16)}
    for key, name in zip(kw, NAMES, strict=True):
        w = jax.random.normal(key, SHAPES[name], jnp.float32) * SHAPES[name][1] ** -0.5
        drawn[name] = (w * {"w_gate": 1.0, "w_up": bump(kh, FF, 4.0), "w_down": layers}[name]).astype(jnp.bfloat16)
    for key, name in zip(km, NAMES, strict=True):
        drawn[f"m_{name}"] = 0.1 * jax.random.normal(key, SHAPES[name], jnp.float32)
    for key, name in zip(kv, NAMES, strict=True):
        drawn[f"v_{name}"] = jax.random.uniform(key, SHAPES[name], jnp.float32, 0.005, 0.015)
    return drawn


def matmul(a, w):
    return jnp.dot(a, w, preferred_element_type=jnp.float32).astype(jnp.bfloat16)


def normed(h):
    wide = h.astype(jnp.float32)
    scale = lax.rsqrt(jnp.mean(wide**2, -1, keepdims=True) + 1e-6)
    return (wide * scale).astype(jnp.bfloat16)


def layer(h, w):
    a = normed(h)
    gate = jnp.dot(a, w["w_gate"], preferred_element_type=jnp.float32)
    up = jnp.dot(a, w["w_up"], preferred_element_type=jnp.float32)
    return h + matmul((jax.nn.silu(gate) * up).astype(jnp.bfloat16), w["w_down"])


def adamw(w, m, v, g):
    m = 0.9 * m + 0.1 * g
    v = 0.95 * v + 0.05 * g * g
    step = m * lax.rsqrt(v + 1e-8) + 0.1 * w
    return (w - 0.02 * step).astype(jnp.bfloat16), m, v


def clipped(gradients, sum_of_squares, count):
    factor = jnp.minimum(1.0, 0.5 * lax.rsqrt(sum_of_squares / count + 1e-30))
    return [g * factor for g in gradients]


def stack(weights, h):
    return lax.scan(lambda h, w: (layer(h, w), None), h, weights)[0]


def reference(x, dy, w_gate, w_up, w_down, m_w_gate, m_w_up, m_w_down, v_w_gate, v_w_up, v_w_down):
    weights = dict(zip(NAMES, (w_gate, w_up, w_down), strict=True))

    def take(so_far, sequence):
        h, by_y = sequence
        _, back = jax.vjp(lambda w: stack(w, h), weights)
        return jax.tree.map(lambda total, term: total + term.astype(jnp.float32), so_far, back(by_y)[0]), None

    none_yet = {name: jnp.zeros(w.shape, jnp.float32) for name, w in weights.items()}
    by_weights, _ = lax.scan(take, none_yet, (x, dy))
    gradients = [by_weights[name].astype(jnp.bfloat16).astype(jnp.float32) for name in NAMES]
    gradients = clipped(gradients, sum(jnp.sum(g * g) for g in gradients), sum(g.size for g in gradients))
    new = [
        adamw(w.astype(jnp.float32), m, v, g)
        for w, m, v, g in zip((w_gate, w_up, w_down), (m_w_gate, m_w_up, m_w_down), (v_w_gate, v_w_up, v_w_down), gradients, strict=True)
    ]
    return tuple(one[which] for which in range(3) for one in new)
```

```python
import functools

import jax
import jax.numpy as jnp
from jax import lax
from jax.experimental import pallas as pl
from jax.experimental.pallas import tpu as pltpu
from jax.sharding import PartitionSpec as P


MESH = pl.DeviceIdType.MESH
BF, F32 = jnp.bfloat16, jnp.float32
ND, NF, NT = 1024, 3200, 2048
COUNT = 6 * ND * NF
TILE = 256
TILES = 13
LAST = NF - TILE
HALF = NF // 2


def chip_of(i):
    chip = i // 2
    y, z = chip // 4, chip % 4
    return z + y * (7 - 2 * z)


def device_at(pos, core):
    row = pos // 4
    return (row * 4 + pos + row * (7 - 2 * pos)) * 2 + core


def rank_of(pos, core):
    return (pos + core * (8 - 2 * pos)) % 8


def place():
    i = lax.axis_index("dp")
    core = i % 2
    pos = chip_of(i)
    step = 1 - 2 * core
    return core, rank_of(pos, core), device_at((pos + step + 8) % 8, core), device_at((pos - step + 8) % 8, core), i + 1 - 2 * core


def reduce_kernel(*refs):
    xs, ys = refs[0:4], refs[4:10]
    gu, gu_mate, dn, dn_mate, factor = refs[10:15]
    xbuf, ybuf, dw, pt, rb, fd, ssq, every, xsem, ysem, psend, precv, ssem, rsem, free, fsend, frecv, esend, erecv = refs[15:]
    core, rank, nxt, _, mate = place()

    barrier = pltpu.get_barrier_semaphore()
    here = lax.axis_index("dp")
    for k in range(1, 16):
        pl.semaphore_signal(barrier, inc=1, device_id={"dp": (here + k) % 16}, device_id_type=MESH)

    def xload(k):
        return pltpu.make_async_copy(xs[k], xbuf.at[k % 2], xsem.at[k % 2])

    def ystart(flat):
        mat, tile = flat // TILES, flat % TILES
        col = pl.multiple_of(jnp.minimum(tile * TILE, LAST), 128)
        for k in range(6):
            @pl.when(mat == k)
            def _():
                pltpu.make_async_copy(ys[k].at[:, pl.ds(col, TILE)], ybuf.at[flat % 3], ysem.at[flat % 3]).start()

    xload(0).start()
    ystart(0)
    ystart(1)
    ssq[...] = jnp.zeros_like(ssq)
    pl.semaphore_wait(barrier, 15)

    def pair(par, part):
        cols = pl.ds(*((0, 1536), (1536, 1024), (2560, 640))[part])
        return pltpu.make_async_remote_copy(
            src_ref=dw.at[par, pl.ds(pl.multiple_of(512 * (1 - core), 512), 512), cols],
            dst_ref=pt.at[par, :, cols],
            send_sem=psend.at[par, part],
            recv_sem=precv.at[par, part],
            device_id={"dp": mate},
            device_id_type=MESH,
        )

    def whole_d(l):
        return pltpu.make_async_remote_copy(
            src_ref=fd.at[0, l],
            dst_ref=fd.at[1, l],
            send_sem=fsend.at[0, l],
            recv_sem=frecv.at[0, l],
            device_id={"dp": mate},
            device_id_type=MESH,
        )

    def whole_gu(k):
        return pltpu.make_async_remote_copy(
            src_ref=gu.at[k],
            dst_ref=gu_mate.at[k],
            send_sem=fsend.at[1, k],
            recv_sem=frecv.at[1, k],
            device_id={"dp": mate},
            device_id_type=MESH,
        )

    def hop(par, s, q):
        return pltpu.make_async_remote_copy(
            src_ref=rb.at[par, s, q],
            dst_ref=rb.at[par, s + 1, q],
            send_sem=ssem.at[par, s, q],
            recv_sem=rsem.at[par, s + 1, q],
            device_id={"dp": nxt},
            device_id_type=MESH,
        )

    def arrival(par, s, q):
        return pltpu.make_async_remote_copy(
            src_ref=rb.at[par, s, q],
            dst_ref=rb.at[par, s, q],
            send_sem=ssem.at[par, s, q],
            recv_sem=rsem.at[par, s, q],
            device_id={"dp": nxt},
            device_id_type=MESH,
        )

    def compute(m, half):
        tile, lower = half // 2, half % 2
        par = m % 2
        flat = m * TILES + tile
        xi = (m // 3) * 2 + jnp.minimum(m % 3, 1)

        @pl.when(lower == 0)
        def _():
            pltpu.make_async_copy(ys[0].at[:, pl.ds(0, TILE)], ybuf.at[flat % 3], ysem.at[flat % 3]).wait()

        rows = pl.ds(pl.multiple_of(lower * 512, 512), 512)
        out = jnp.dot(xbuf[xi % 2, rows, :], ybuf[flat % 3], preferred_element_type=F32).astype(BF)
        col = pl.multiple_of(jnp.minimum(tile * TILE, LAST), 128)
        dw[par, rows, pl.ds(col, TILE)] = out

        @pl.when((lower == 1) & (flat + 2 < 6 * TILES) )
        def _():
            ystart(flat + 2)

    def stage(m, carry):
        par = (m + 1) % 2

        @pl.when((m == 0) | (m == 1) | (m == 3) | (m == 4))
        def _():
            k = (m // 3) % 2 * 2 + jnp.minimum(m % 3, 1)
            pltpu.make_async_copy(xs[0], xbuf.at[k % 2], xsem.at[k % 2]).wait()

        for when, k in ((0, 1), (2, 2), (3, 3)):
            @pl.when(m == when)
            def _():
                xload(k).start()

        @pl.when((m >= 1) & (m < 7))
        def _():
            for part in range(3):
                pair(par, part).wait()

        def slot(n, carry):
            late = jnp.minimum(n // 4, 1)
            s = late * ((n - 2) // 4)
            q = (n + 2 * late) % 4

            @pl.when((m >= 1) & (m < 7) & (n != 4) & (n != 5))
            def _():
                shard = (rank + 7 - s) % 8
                row = pl.multiple_of(64 * shard + 16 * q, 16)
                mine = dw[par, pl.ds(pl.multiple_of(512 * core + row, 16), 16), :].astype(F32) + pt[par, pl.ds(row, 16), :].astype(F32)

                @pl.when(s == 0)
                def _():
                    rb[par, 0, q] = mine.astype(BF)

                @pl.when(s > 0)
                def _():
                    arrival(par, s, q).wait_recv()
                    rb[par, s, q] = (rb[par, s, q].astype(F32) + mine).astype(BF)

            @pl.when((m >= 2) & (n == 4))
            def _():
                old = 1 - par
                for k in range(4):
                    row = pl.multiple_of(64 * rank + 16 * k, 16)
                    mine = dw[old, pl.ds(pl.multiple_of(512 * core + row, 16), 16), :].astype(F32) + pt[old, pl.ds(row, 16), :].astype(F32)
                    arrival(old, 7, k).wait_recv()
                    g = (rb[old, 7, k].astype(F32) + mine).astype(BF)

                    @pl.when((m == 2) | (m == 5))
                    def _():
                        fd[0, m // 3, 16 * k : 16 * k + 16, :] = g

                    @pl.when((m != 2) & (m != 5))
                    def _():
                        gu[(m - 3) - (m // 5), 16 * k : 16 * k + 16, :] = g

                    wide = g.astype(F32)
                    ssq[...] += jnp.sum((wide * wide).reshape(2, 8, 25, 128), axis=(0, 2))
                    hop(old, 6, k).wait_send()

                @pl.when(m < 6)
                def _():
                    pl.semaphore_signal(free, inc=1, device_id={"dp": mate}, device_id_type=MESH)

            @pl.when((m < 6) & (n >= 4))
            def _():
                compute(m, n - 4)

            @pl.when(((m == 2) | (m == 5)) & (n == 5))
            def _():
                whole_d(m // 3).start()

            @pl.when(((m == 3) | (m == 4) | (m >= 6)) & (n == 5))
            def _():
                whole_gu((m - 3) - (m // 5)).start()

            @pl.when(((m == 2) | (m == 5)) & (n == 25))
            def _():
                l = m // 3
                whole_d(l).wait()
                both = jnp.concatenate([fd[core, l], fd[1 - core, l]], axis=0)
                for c in range(2):
                    @pl.when(core == c)
                    def _():
                        dn[l] = both[:, c * HALF : (c + 1) * HALF].T
                        dn_mate[l] = both[:, (1 - c) * HALF : (2 - c) * HALF].T

            @pl.when((m < 6) & (n == 15))
            def _():
                @pl.when(m >= 2)
                def _():
                    pl.semaphore_wait(free, 1)

                pair(m % 2, 0).start()

            @pl.when((m < 6) & (n == 23))
            def _():
                pair(m % 2, 1).start()

            @pl.when((m < 6) & (n == 29))
            def _():
                pair(m % 2, 2).start()

            @pl.when((m >= 1) & (m < 7) & (n != 4) & (n != 5))
            def _():
                hop(par, s, q).start()

                @pl.when(s > 0)
                def _():
                    hop(par, s - 1, q).wait_send()

            return carry

        return lax.fori_loop(0, 30, slot, carry)

    lax.fori_loop(0, 8, stage, 0)

    every[here] = ssq[...]

    def tell(k):
        return pltpu.make_async_remote_copy(
            src_ref=every.at[here],
            dst_ref=every.at[here],
            send_sem=esend.at[k],
            recv_sem=erecv.at[k],
            device_id={"dp": (here + k) % 16},
            device_id_type=MESH,
        )

    for k in range(1, 16):
        tell(k).start()
    for k in range(4):
        whole_gu(k).wait()
    for k in range(1, 16):
        pltpu.make_async_remote_copy(
            src_ref=every.at[here],
            dst_ref=every.at[(here + 16 - k) % 16],
            send_sem=esend.at[k],
            recv_sem=erecv.at[k],
            device_id={"dp": (here + k) % 16},
            device_id_type=MESH,
        ).wait()
    total = every[0]
    for k in range(1, 16):
        total = total + every[k]
    total = jnp.sum(jnp.sum(total, axis=1, keepdims=True), axis=0, keepdims=True)
    factor[...] = jnp.broadcast_to(jnp.minimum(1.0, 0.5 * lax.rsqrt(total / COUNT + 1e-30)), factor.shape)


def reduce_call(xs, ys):
    return pl.pallas_call(
        reduce_kernel,
        out_shape=(
            jax.ShapeDtypeStruct((4, 64, NF), BF),
            jax.ShapeDtypeStruct((4, 64, NF), BF),
            jax.ShapeDtypeStruct((2, HALF, 128), BF),
            jax.ShapeDtypeStruct((2, HALF, 128), BF),
            jax.ShapeDtypeStruct((8, 128), F32),
        ),
        in_specs=[pl.BlockSpec(memory_space=pl.ANY)] * 10,
        out_specs=(pl.BlockSpec(memory_space=pltpu.VMEM),) * 5,
        scratch_shapes=[
            pltpu.VMEM((2, ND, NT), BF),
            pltpu.VMEM((3, NT, TILE), BF),
            pltpu.VMEM((2, ND, NF), BF),
            pltpu.VMEM((2, ND // 2, NF), BF),
            pltpu.VMEM((2, 8, 4, 16, NF), BF),
            pltpu.VMEM((2, 2, 64, NF), BF),
            pltpu.VMEM((8, 128), F32),
            pltpu.VMEM((16, 8, 128), F32),
            pltpu.SemaphoreType.DMA((2,)),
            pltpu.SemaphoreType.DMA((3,)),
            pltpu.SemaphoreType.DMA((2, 3)),
            pltpu.SemaphoreType.DMA((2, 3)),
            pltpu.SemaphoreType.DMA((2, 8, 4)),
            pltpu.SemaphoreType.DMA((2, 8, 4)),
            pltpu.SemaphoreType.REGULAR,
            pltpu.SemaphoreType.DMA((2, 4)),
            pltpu.SemaphoreType.DMA((2, 4)),
            pltpu.SemaphoreType.DMA((16,)),
            pltpu.SemaphoreType.DMA((16,)),
        ],
        compiler_params=pltpu.CompilerParams(collective_id=0, has_side_effects=True, vmem_limit_bytes=60 << 20),
        name="reduce",
    )(*xs, *ys)


def adamw_kernel(first, where, factor, *refs):
    own_gu, mate_gu, own_dn, mate_dn = refs[0:4]
    ins = refs[4:13]
    outs = refs[13:22] if first else refs[22:31]
    f = factor[0, 0]
    side = pl.program_id(0)
    for c in range(2):

        @pl.when(side == c)
        def _():
            gu, dn = ((own_gu, own_dn), (mate_gu, mate_dn))[c]
            for k in range(3):
                g = (gu[0, k] if k < 2 else dn[0]).astype(F32) * f
                m = 0.9 * ins[3 + k][0] + 0.1 * g
                v = 0.95 * ins[6 + k][0] + 0.05 * g * g
                wide = ins[k][0].astype(F32)
                outs[k][0] = (wide - 0.02 * (m * lax.rsqrt(v + 1e-8) + 0.1 * wide)).astype(BF)
                outs[3 + k][0] = m
                outs[6 + k][0] = v


def adamw_call(where, factor, grads, state, new, parts=2):
    first = new is None
    gu_rows, dn_rows = 64 // parts, HALF // parts

    def gu_spec(side):
        return pl.BlockSpec((1, 2, gu_rows, NF), lambda c, l, j, w: (jnp.where(c == side, l, 1 - side), 0, jnp.where(c == side, j, (1 - side) * (parts - 1)), 0))

    def dn_spec(side):
        return pl.BlockSpec((1, dn_rows, 128), lambda c, l, j, w: (jnp.where(c == side, l, 1 - side), jnp.where(c == side, j, (1 - side) * (parts - 1)), 0))

    wide = pl.BlockSpec((1, gu_rows, NF), lambda c, l, j, w: (1 - l, w[c] * parts + j, 0))
    tall = pl.BlockSpec((1, dn_rows, 128), lambda c, l, j, w: (1 - l, w[4 + c] * parts + j, w[2 + c]))
    blocks = [wide, wide, tall] * 3
    anywhere = [] if first else [pl.BlockSpec(memory_space=pl.ANY)] * 9
    shapes = [jax.ShapeDtypeStruct(a.shape, a.dtype) for a in state]
    return pl.pallas_call(
        functools.partial(adamw_kernel, first),
        out_shape=shapes,
        grid_spec=pltpu.PrefetchScalarGridSpec(
            num_scalar_prefetch=1,
            grid=(2, 2, parts),
            in_specs=[pl.BlockSpec(memory_space=pltpu.SMEM), gu_spec(0), gu_spec(1), dn_spec(0), dn_spec(1), *blocks, *anywhere],
            out_specs=blocks,
        ),
        input_output_aliases={} if first else {15 + k: k for k in range(9)},
        compiler_params=pltpu.CompilerParams(vmem_limit_bytes=40 << 20),
        cost_estimate=pl.CostEstimate(flops=int(8e9), bytes_accessed=54 << 20, transcendentals=0),
        name="adamw",
    )(where, factor, *grads, *state, *([] if first else new))


def normed(h):
    wide = h.astype(F32)
    scale = lax.rsqrt(jnp.mean(wide**2, -1, keepdims=True) + 1e-6)
    return (wide * scale).astype(BF), scale


def dot(a, b):
    return jnp.dot(a, b, preferred_element_type=F32)


def backward_act(gate, up, dact):
    dact = dact.astype(F32)
    s = jax.nn.sigmoid(gate)
    return (dact * up * (s + gate * s * (1 - s))).astype(BF), (dact * gate * s).astype(BF)


def front(x, dy, w_gate, w_up, w_down):
    a0, _ = normed(x)
    gate0, up0 = dot(a0, w_gate[0]), dot(a0, w_up[0])
    act0 = (jax.nn.silu(gate0) * up0).astype(BF)
    h1 = x + dot(act0, w_down[0]).astype(BF)
    a1, scale = normed(h1)
    gate1, up1 = dot(a1, w_gate[1]), dot(a1, w_up[1])
    act1 = (jax.nn.silu(gate1) * up1).astype(BF)
    dgate1, dup1 = backward_act(gate1, up1, dot(dy, w_down[1].T).astype(BF))
    da = (dot(dgate1, w_gate[1].T).astype(BF) + dot(dup1, w_up[1].T).astype(BF)).astype(F32)
    wide = h1.astype(F32)
    dh = (da * scale - wide * scale**3 * jnp.mean(da * wide, -1, keepdims=True)).astype(BF) + dy
    dgate0, dup0 = backward_act(gate0, up0, dot(dh, w_down[0].T).astype(BF))

    def turned(d):
        t = d.T.reshape(8, 2, 64, NT)
        return jnp.concatenate([t[:, 0], t[jnp.array([(8 - k) % 8 for k in range(8)]), 1]]).reshape(ND, NT)

    return (turned(dy), a1.T, turned(dh), a0.T), (act1, dgate1, dup1, act0, dgate0, dup0)


RING = [(device_at(p, 0), device_at((p + 1) % 8, 0)) for p in range(8)] + [(device_at(p, 1), device_at((p + 7) % 8, 1)) for p in range(8)]
MATE = [(i, i ^ 1) for i in range(16)]


def solution(mesh):
    def step(x, dy, *state):
        xs, ys = front(x[0], dy[0], *state[:3])
        gu, gu_mate, dn, dn_mate, factor = reduce_call(xs, ys)
        gu, gu_mate = gu.reshape(2, 2, 64, NF), gu_mate.reshape(2, 2, 64, NF)
        core, rank, *_ = place()
        pos = chip_of(lax.axis_index("dp"))
        other = rank_of(pos, 1 - core)
        new = None
        for s in range(8):
            mine, its = (rank - s) % 8, (other - s) % 8
            where = jnp.stack([8 * core + mine, 8 * (1 - core) + its, rank_of(mine, core), rank_of(its, 1 - core), core, 1 - core]).astype(jnp.int32)
            if s:
                gu = lax.ppermute(gu, "dp", RING)
                dn = lax.ppermute(dn, "dp", RING)
                gu_mate = lax.ppermute(gu, "dp", MATE)
                dn_mate = lax.ppermute(dn, "dp", MATE)
            new = adamw_call(where, factor[:1, :1], (gu, gu_mate, dn, dn_mate), state, new)
        return tuple(new)

    return jax.shard_map(
        step,
        mesh=mesh,
        in_specs=(P(("rep", "dp"), None, None),) * 2 + (P(None, None, None),) * 9,
        out_specs=(P("rep", None, None),) * 9,
        check_vma=False,
    )
```

```python
import jax
import jax.numpy as jnp
from jax import lax
from jax.experimental import pallas as pl
from jax.experimental.pallas import tpu as pltpu
from jax.sharding import PartitionSpec as P


MESH = pl.DeviceIdType.MESH
BF, F32 = jnp.bfloat16, jnp.float32
ND, NF, NT = 1024, 3200, 2048
COUNT = 6 * ND * NF
TILE = 256
TILES = 13
LAST = NF - TILE
HALF = NF // 2
ROWS = 16
GROUP = 16
OTHERS = range(1, GROUP)
LANES = 128
RUN = 64


def chip_of(i):
    chip = i // 2
    y, z = chip // 4, chip % 4
    return z + y * (7 - 2 * z)


def device_at(pos, core):
    row = pos // 4
    return (row * 4 + pos + row * (7 - 2 * pos)) * 2 + core


def rank_of(pos, core):
    return (pos + core * (8 - 2 * pos)) % 8


def place():
    i = lax.axis_index("dp")
    core = i % 2
    pos = chip_of(i)
    step = 1 - 2 * core
    return core, rank_of(pos, core), device_at((pos + step + 8) % 8, core), device_at((pos - step + 8) % 8, core), i + 1 - 2 * core


def reduce_kernel(*refs):
    dy, a1, dh1, a0, act1, dgate1, dup1, act0, gate, up, wd = refs[0:11]
    gu, gu_mate, dn, dn_mate, factor, dgate0, dup0 = refs[11:18]
    xnat, xbuf, ybuf, dw, pt, rb, fd, ssq, every, wdb, gub, ob = refs[18:30]
    xsem, ysem, psend, precv, ssem, rsem, free, fsend, frecv, esend, erecv, isem, osem = refs[30:]
    ys = (act1, dgate1, dup1, act0, dgate0, dup0)
    core, rank, nxt, _, mate = place()

    barrier = pltpu.get_barrier_semaphore()
    here = lax.axis_index("dp")
    for k in OTHERS:
        pl.semaphore_signal(barrier, inc=1, device_id={"dp": (here + k) % GROUP}, device_id_type=MESH)

    def xload(src):
        return pltpu.make_async_copy(src, xnat, xsem)

    def turn(k, ordered):
        for j in range(8):
            both = slice(LANES * j, LANES * (j + 1))
            part = xnat[:, both].T
            if ordered:
                there = (8 - j) % 8 + 8
                xbuf[k, RUN * j : RUN * (j + 1), :] = part[:RUN]
                xbuf[k, RUN * there : RUN * (there + 1), :] = part[RUN:]
            else:
                xbuf[k, both, :] = part

    def tile_col(tile):
        return pl.multiple_of(jnp.minimum(tile * TILE, LAST), 128)

    def yload(src, flat):
        return pltpu.make_async_copy(src.at[:, pl.ds(tile_col(flat % TILES), TILE)], ybuf.at[flat % 3], ysem.at[flat % 3])

    def ystart(flat):
        for k in range(6):

            @pl.when(flat // TILES == k)
            def _():
                yload(ys[k], flat).start()

    def unit_place(v):
        return pl.ds(pl.multiple_of(v // 7 * WIDE, WIDE), WIDE), pl.ds(pl.multiple_of(jnp.minimum(v % 7 * WIDE, NF - WIDE), 128), WIDE)

    def unit_loads(v):
        rows, cols = unit_place(v)
        slot = v % 2
        return [
            pltpu.make_async_copy(wd.at[0, cols], wdb.at[slot], isem.at[slot, 0]),
            pltpu.make_async_copy(gate.at[rows, cols], gub.at[slot, 0], isem.at[slot, 1]),
            pltpu.make_async_copy(up.at[rows, cols], gub.at[slot, 1], isem.at[slot, 2]),
        ]

    def unit_stores(v):
        slot = v % 2
        return [pltpu.make_async_copy(ob.at[slot, k], dst.at[unit_place(v)], osem.at[slot, k]) for k, dst in enumerate((dgate0, dup0))]

    def unit(v):
        @pl.when(v >= 2)
        def _():
            for copy in unit_stores(v - 2):
                copy.wait()

        @pl.when((v >= 1) & (v < 29))
        def _():
            for copy in unit_stores(v - 1):
                copy.start()

        @pl.when(v < 28)
        def _():
            for copy in unit_loads(v):
                copy.wait()
            slot = v % 2
            d = dot_t(xnat[unit_place(v)[0], :], wdb[slot]).astype(BF).astype(F32)
            g, u = gub[slot, 0], gub[slot, 1]
            s, gated = silu_parts(g)
            ob[slot, 0] = (d * u * (s + gated * (1 - s))).astype(BF)
            ob[slot, 1] = (d * gated).astype(BF)

        @pl.when(v + 2 < 28)
        def _():
            for copy in unit_loads(v + 2):
                copy.start()

    xload(dy).start()
    ystart(0)
    ystart(1)
    for copy in unit_loads(0) + unit_loads(1):
        copy.start()
    ssq[...] = jnp.zeros_like(ssq)
    pl.semaphore_wait(barrier, len(OTHERS))

    def pair(par, part):
        cols = pl.ds(*((0, 1536), (1536, 1024), (2560, 640))[part])
        return pltpu.make_async_remote_copy(
            src_ref=dw.at[par, pl.ds(pl.multiple_of(512 * (1 - core), 512), 512), cols],
            dst_ref=pt.at[par, :, cols],
            send_sem=psend.at[par, part],
            recv_sem=precv.at[par, part],
            device_id={"dp": mate},
            device_id_type=MESH,
        )

    def whole_d(l):
        return pltpu.make_async_remote_copy(
            src_ref=fd.at[0, l],
            dst_ref=fd.at[1, l],
            send_sem=fsend.at[0, l],
            recv_sem=frecv.at[0, l],
            device_id={"dp": mate},
            device_id_type=MESH,
        )

    def whole_gu(k):
        return pltpu.make_async_remote_copy(
            src_ref=gu.at[k],
            dst_ref=gu_mate.at[k],
            send_sem=fsend.at[1, k],
            recv_sem=frecv.at[1, k],
            device_id={"dp": mate},
            device_id_type=MESH,
        )

    def hop(par, s, q):
        return pltpu.make_async_remote_copy(
            src_ref=rb.at[par, s, q],
            dst_ref=rb.at[par, s + 1, q],
            send_sem=ssem.at[par, s, q],
            recv_sem=rsem.at[par, s + 1, q],
            device_id={"dp": nxt},
            device_id_type=MESH,
        )

    def arrival(par, s, q):
        return pltpu.make_async_remote_copy(
            src_ref=rb.at[par, s, q],
            dst_ref=rb.at[par, s, q],
            send_sem=ssem.at[par, s, q],
            recv_sem=rsem.at[par, s, q],
            device_id={"dp": nxt},
            device_id_type=MESH,
        )

    def compute(m, tile):
        flat = m * TILES + tile
        yload(act1, flat).wait()
        dw[m % 2, :, pl.ds(tile_col(tile), TILE)] = dot(xbuf[jnp.minimum(m % 3, 1)], ybuf[flat % 3]).astype(BF)

        @pl.when(flat + 2 < 6 * TILES)
        def _():
            ystart(flat + 2)

    def own_part(par, shard, q):
        row = pl.multiple_of(RUN * (shard % 8) + ROWS * q, ROWS)
        here = pl.multiple_of(512 * core + row, ROWS)
        return dw[par, pl.ds(here, ROWS), :].astype(F32) + pt[par, pl.ds(row, ROWS), :].astype(F32)

    def stage(m, carry):
        par = (m + 1) % 2
        making, summing = m < 6, (m >= 1) & (m < 7)
        ended = m - 2
        ends_down = m % 3 == 2
        ends_wide = (ended >= 0) & ~ends_down
        layer = m // 3
        wide_slot = ended - 1 - m // 5
        new_down = making & (m % 3 == 0)
        new_wide = (m == 1) | (m == 4)

        @pl.when((m == 0) | new_wide)
        def _():
            xload(dy).wait()

        @pl.when(new_down)
        def _():
            turn(0, True)

        @pl.when(new_wide)
        def _():
            turn(1, False)

        for when, src in ((0, a1), (1, dh1)):

            @pl.when(m == when)
            def _():
                xload(src).start()

        @pl.when(summing)
        def _():
            for part in range(3):
                pair(par, part).wait()

        def slot(n, carry):
            late = jnp.minimum(n // 4, 1)
            s = late * ((n - 2) // 4)
            q = (n + 2 * late) % 4
            odd = n % 2 == 1
            ringing = summing & (n // 2 != 2)

            @pl.when(ringing)
            def _():
                mine = own_part(par, rank + 7 - s, q)

                @pl.when(s == 0)
                def _():
                    rb[par, 0, q] = mine.astype(BF)

                @pl.when(s > 0)
                def _():
                    arrival(par, s, q).wait_recv()
                    rb[par, s, q] = (rb[par, s, q].astype(F32) + mine).astype(BF)

            @pl.when((ended >= 0) & (n == 4))
            def _():
                old = 1 - par
                for k in range(4):
                    rows = slice(ROWS * k, ROWS * k + ROWS)
                    mine = own_part(old, rank, k)
                    arrival(old, 7, k).wait_recv()
                    g = (rb[old, 7, k].astype(F32) + mine).astype(BF)

                    @pl.when(ends_down)
                    def _():
                        fd[0, layer, rows, :] = g

                    @pl.when(ends_wide)
                    def _():
                        gu[wide_slot, rows, :] = g

                    wide = g.astype(F32)
                    ssq[...] += jnp.sum((wide * wide).reshape(2, 8, 25, 128), axis=(0, 2))
                    hop(old, 6, k).wait_send()

                @pl.when(making)
                def _():
                    pl.semaphore_signal(free, inc=1, device_id={"dp": mate}, device_id_type=MESH)

            @pl.when(ringing)
            def _():
                @pl.when(s > 0)
                def _():
                    hop(par, s - 1, q).wait_send()

                hop(par, s, q).start()

            @pl.when(making & (n >= 4) & (n < 26) & (~odd | (n >= 23)))
            def _():
                compute(m, n // 2 - 2 + n // 23 * (n - 11 - n // 2))

            @pl.when(summing & (layer * m < 4) & (n >= 5) & odd & (n < 24))
            def _():
                @pl.when((m == 1) & (n == 5))
                def _():
                    xload(dh1).wait()

                unit(10 * (m - 1) + n // 2 - 2)

            @pl.when((n == 5) | (n == 15) | (n >= 23))
            def _():
                @pl.when((m == 3) & (n == 25))
                def _():
                    xload(a0).start()

                @pl.when(ends_down & (n == 5))
                def _():
                    whole_d(layer).start()

                @pl.when(ends_wide & (n == 5))
                def _():
                    whole_gu(wide_slot).start()

                @pl.when(ends_down & (n == 25))
                def _():
                    whole_d(layer).wait()
                    both = jnp.concatenate([fd[core, layer], fd[1 - core, layer]], axis=0)
                    for c, (mine, its) in enumerate(((dn, dn_mate), (dn_mate, dn))):

                        @pl.when(core == c)
                        def _():
                            mine[layer] = both[:, :HALF].T
                            its[layer] = both[:, HALF:].T

                for when, part in ((15, 0), (23, 1), (26, 2)):

                    @pl.when(making & (n == when))
                    def _():
                        if part == 0:

                            @pl.when(ended >= 0)
                            def _():
                                pl.semaphore_wait(free, 1)

                        pair(1 - par, part).start()

            return carry

        return lax.fori_loop(0, 30 - 24 * (m // 7), slot, carry)

    lax.fori_loop(0, 8, stage, 0)

    every[here] = ssq[...]

    def tell(k):
        return pltpu.make_async_remote_copy(
            src_ref=every.at[here],
            dst_ref=every.at[here],
            send_sem=esend.at[k],
            recv_sem=erecv.at[k],
            device_id={"dp": (here + k) % GROUP},
            device_id_type=MESH,
        )

    for k in OTHERS:
        tell(k).start()
    for k in range(4):
        whole_gu(k).wait()
    for k in OTHERS:
        pltpu.make_async_remote_copy(
            src_ref=every.at[here],
            dst_ref=every.at[(here + GROUP - k) % GROUP],
            send_sem=esend.at[k],
            recv_sem=erecv.at[k],
            device_id={"dp": (here + k) % GROUP},
            device_id_type=MESH,
        ).wait()
    total = every[0]
    for k in OTHERS:
        total = total + every[k]
    total = jnp.sum(jnp.sum(total, axis=1, keepdims=True), axis=0, keepdims=True)
    factor[...] = jnp.broadcast_to(jnp.minimum(1.0, 0.5 * lax.rsqrt(total / COUNT + 1e-30)), factor.shape)


def reduce_call(*arrays):
    vmem, dma = pltpu.VMEM, pltpu.SemaphoreType.DMA
    own = pl.BlockSpec(memory_space=pltpu.VMEM)
    anywhere = pl.BlockSpec(memory_space=pl.ANY)
    return pl.pallas_call(
        reduce_kernel,
        out_shape=[jax.ShapeDtypeStruct((4, RUN, NF), BF)] * 2
        + [jax.ShapeDtypeStruct((2, HALF, LANES), BF)] * 2
        + [jax.ShapeDtypeStruct((8, LANES), F32)]
        + [jax.ShapeDtypeStruct((NT, NF), BF)] * 2,
        in_specs=[anywhere] * 11,
        out_specs=[own] * 5 + [anywhere] * 2,
        scratch_shapes=[
            vmem((NT, ND), BF),
            vmem((2, ND, NT), BF),
            vmem((3, NT, TILE), BF),
            vmem((2, ND, NF), BF),
            vmem((2, ND // 2, NF), BF),
            vmem((2, 8, 4, ROWS, NF), BF),
            vmem((2, 2, RUN, NF), BF),
            vmem((8, LANES), F32),
            vmem((16, 8, LANES), F32),
            vmem((2, WIDE, ND), BF),
            *[vmem((2, 2, WIDE, WIDE), t) for t in (F32, BF)],
            dma(()),
            dma((3,)),
            *[dma((2, 3))] * 2,
            *[dma((2, 8, 4))] * 2,
            pltpu.SemaphoreType.REGULAR,
            *[dma((2, 4))] * 2,
            *[dma((16,))] * 2,
            *[dma((2, 3))] * 2,
        ],
        compiler_params=pltpu.CompilerParams(collective_id=0, has_side_effects=True, vmem_limit_bytes=67043328),
        name="reduce",
    )(*arrays)


def adamw_kernel(where, factor, *refs):
    sides = (refs[0], refs[2]), (refs[1], refs[3])
    ins, outs = refs[4:13], refs[-11:-2]
    gu, dn = refs[-2:]
    f = factor[0, 0]
    for c, (gu_side, dn_side) in enumerate(sides):

        @pl.when(pl.program_id(0) == c)
        def _():
            gu[...] = gu_side[0]
            dn[...] = dn_side[0]

    def some(i, carry):
        for k in range(3):
            whole = ins[k].shape[1]
            rows = pl.ds(pl.multiple_of(i * (whole // 2), ROWS), whole // 2)
            w_in, m_in, v_in = ins[k::3]
            w_out, m_out, v_out = outs[k::3]
            g = (dn[rows] if k == 2 else gu[k, rows]).astype(F32) * f
            m = 0.9 * m_in[0, rows] + 0.1 * g
            v = 0.95 * v_in[0, rows] + 0.05 * g * g
            wide = w_in[0, rows].astype(F32)
            w_out[0, rows] = (wide - 0.02 * (m * lax.rsqrt(v + 1e-8) + 0.1 * wide)).astype(BF)
            m_out[0, rows] = m
            v_out[0, rows] = v
        return carry

    lax.fori_loop(0, 2, some, 0)


def adamw_call(where, factor, grads, state, new, parts=2):
    first = new is None
    gu_rows, dn_rows = 64 // parts, HALF // parts

    def gu_spec(side):
        return pl.BlockSpec((1, 2, gu_rows, NF), lambda c, l, j, w: (jnp.where(c == side, l, 1 - side), 0, jnp.where(c == side, j, (1 - side) * (parts - 1)), 0))

    def dn_spec(side):
        return pl.BlockSpec((1, dn_rows, 128), lambda c, l, j, w: (jnp.where(c == side, l, 1 - side), jnp.where(c == side, j, (1 - side) * (parts - 1)), 0))

    wide = pl.BlockSpec((1, gu_rows, NF), lambda c, l, j, w: (1 - l, w[c] * parts + j, 0))
    tall = pl.BlockSpec((1, dn_rows, 128), lambda c, l, j, w: (1 - l, w[4 + c] * parts + j, w[2 + c]))
    blocks = [wide, wide, tall] * 3
    anywhere = [] if first else [pl.BlockSpec(memory_space=pl.ANY)] * 9
    shapes = [jax.ShapeDtypeStruct(a.shape, a.dtype) for a in state]
    return pl.pallas_call(
        adamw_kernel,
        out_shape=shapes,
        grid_spec=pltpu.PrefetchScalarGridSpec(
            num_scalar_prefetch=1,
            grid=(2, 2, parts),
            in_specs=[pl.BlockSpec(memory_space=pltpu.SMEM), gu_spec(0), gu_spec(1), dn_spec(0), dn_spec(1), *blocks, *anywhere],
            out_specs=blocks,
            scratch_shapes=[pltpu.VMEM((2, gu_rows, NF), BF), pltpu.VMEM((dn_rows, 128), BF)],
        ),
        input_output_aliases={} if first else {15 + k: k for k in range(9)},
        compiler_params=pltpu.CompilerParams(vmem_limit_bytes=40 << 20),
        cost_estimate=pl.CostEstimate(flops=int(8e9), bytes_accessed=54 << 20, transcendentals=0),
        name="adamw",
    )(where, factor, *grads, *state, *([] if first else new))


def norm_scale(wide):
    return lax.rsqrt(jnp.mean(wide * wide, -1, keepdims=True) + 1e-6)


def dot_of(a, b, contracted):
    return lax.dot_general(a, b, (((contracted,), (contracted,)), ((), ())), preferred_element_type=F32)


def dot(a, b):
    return jnp.dot(a, b, preferred_element_type=F32)


def dot_t(a, b):
    return dot_of(a, b, 1)


def at_first(copies):
    begin = pl.program_id(0) == 0

    @pl.when(begin)
    def _():
        for copy in copies:
            copy.start()

    def need(*which):
        @pl.when(begin)
        def _():
            for k in which:
                copies[k].wait()

    return need


def silu_parts(g):
    s = jax.nn.sigmoid(g)
    return s, g * s


WIDE = 512
WHOLE = NF // WIDE
TAIL = WHOLE * WIDE
EDGE = NF - TAIL
CUTS = [(c * WIDE, WIDE) for c in range(WHOLE)] + [(TAIL, EDGE)]


def first_kernel(x, wg_hbm, wu_hbm, wd_hbm, gate, up, act, h, a_ref, wg, wu, wd, wsem):
    copies = []
    for k, (col, n) in enumerate(CUTS):
        for j, (src, dst) in enumerate(((wg_hbm, wg), (wu_hbm, wu))):
            copies.append(pltpu.make_async_copy(src.at[0, :, pl.ds(col, n)], dst.at[:, pl.ds(col, n)], wsem.at[j, k]))
    copies.append(pltpu.make_async_copy(wd_hbm.at[0], wd, wsem.at[2, 0]))
    need = at_first(copies)
    wide = x[...].astype(F32)
    a_ref[...] = (wide * norm_scale(wide)).astype(BF)

    def finish(col, n):
        g, u = gate[:, col : col + n], up[:, col : col + n]
        act[:, col : col + n] = (silu_parts(g)[1] * u).astype(BF)

    for c in range(WHOLE):
        if c % 2 == 0:
            need(*range(2 * c, 2 * c + 4))
        cols = slice(c * WIDE, (c + 1) * WIDE)
        gate[:, cols] = dot(a_ref[...], wg[:, cols])
        up[:, cols] = dot(a_ref[...], wu[:, cols])
        if c:
            finish((c - 1) * WIDE, WIDE)
    need(*range(2 * WHOLE, len(copies)))
    both = dot(a_ref[...], jnp.concatenate([wg[:, TAIL:], wu[:, TAIL:]], axis=1))
    gate[:, TAIL:] = both[:, :EDGE]
    up[:, TAIL:] = both[:, EDGE:]
    finish(TAIL - WIDE, WIDE)
    finish(TAIL, EDGE)
    for n in range(0, ND, WIDE):
        cols = slice(n, n + WIDE)
        h[:, cols] = x[:, cols] + dot(act[...], wd[:, cols]).astype(BF)


def second_kernel(h, dy, wg_hbm, wu_hbm, wd_hbm, act, dgate, dup, dh, a_ref, wg, wu, wd, gs, us, ds, wsem):
    copies = []
    for k, (col, n) in enumerate(CUTS):
        for j, (src, dst) in enumerate(((wg_hbm, wg), (wu_hbm, wu))):
            copies.append(pltpu.make_async_copy(src.at[1, :, pl.ds(col, n)], dst.at[:, pl.ds(col, n)], wsem.at[j, k]))
        copies.append(pltpu.make_async_copy(wd_hbm.at[1, pl.ds(col, n), :], wd.at[pl.ds(col, n), :], wsem.at[2, k]))
    need = at_first(copies)
    wide = h[...].astype(F32)
    a_ref[...] = (wide * norm_scale(wide)).astype(BF)

    def finish(slot, col, n):
        g, u, d = gs[slot, :, :n], us[slot, :, :n], ds[slot, :, :n].astype(BF).astype(F32)
        s, gated = silu_parts(g)
        cols = pl.ds(col, n)
        act[:, cols] = (gated * u).astype(BF)
        dup[:, cols] = (d * gated).astype(BF)
        dgate[:, cols] = (d * u * (s + gated * (1 - s))).astype(BF)

    def pair(p, carry):
        for k in range(WHOLE // 2):

            @pl.when(p == k)
            def _():
                need(*range(6 * k, 6 * k + 6))

        for slot in range(2):
            cols = pl.ds(pl.multiple_of((2 * p + slot) * WIDE, WIDE), WIDE)
            gs[slot] = dot(a_ref[...], wg[:, cols])
            us[slot] = dot(a_ref[...], wu[:, cols])
            ds[slot] = dot_t(dy[...], wd[cols, :])
            finish(1 - slot, pl.multiple_of(jnp.maximum(2 * p + slot - 1, 0) * WIDE, WIDE), WIDE)
        return carry

    lax.fori_loop(0, WHOLE // 2, pair, 0)
    need(*range(3 * WHOLE, len(copies)))
    both = dot(a_ref[...], jnp.concatenate([wg[:, TAIL:], wu[:, TAIL:]], axis=1))
    gs[0, :, :EDGE] = both[:, :EDGE]
    us[0, :, :EDGE] = both[:, EDGE:]
    ds[0, :, :EDGE] = dot_t(dy[...], wd[TAIL:, :])
    finish(1, TAIL - WIDE, WIDE)
    finish(0, TAIL, EDGE)

    def half(k, carry):
        cols = pl.ds(pl.multiple_of(k * WIDE, WIDE), WIDE)
        dh[:, cols] = dot_t(dgate[...], wg[cols, :]).astype(BF) + dot_t(dup[...], wu[cols, :]).astype(BF)
        return carry

    lax.fori_loop(0, 2, half, 0)

    def normal(k, carry):
        rows = pl.ds(pl.multiple_of(k * LANES, LANES), LANES)
        da = dh[rows].astype(F32)
        wide = h[rows].astype(F32)
        scale = norm_scale(wide)
        back = da * scale - wide * (scale * scale * scale * jnp.mean(da * wide, -1, keepdims=True))
        dh[rows] = back.astype(BF) + dy[rows]
        return carry

    lax.fori_loop(0, h.shape[0] // LANES, normal, 0)


def by_tokens(kernel, ins, weights, outs, scratch, rows=WIDE):
    return pl.pallas_call(
        kernel,
        grid=(NT // rows,),
        out_shape=[jax.ShapeDtypeStruct((NT, int(n)), F32 if isinstance(n, float) else BF) for n in outs],
        in_specs=[pl.BlockSpec((rows, a.shape[1]), lambda i: (i, 0)) for a in ins] + [pl.BlockSpec(memory_space=pl.ANY)] * len(weights),
        out_specs=[pl.BlockSpec((rows, int(n)), lambda i: (i, 0)) for n in outs],
        scratch_shapes=scratch,
        compiler_params=pltpu.CompilerParams(vmem_limit_bytes=67043328),
    )(*ins, *weights)


def front(x, dy, weights):
    vmem, sem = pltpu.VMEM, pltpu.SemaphoreType.DMA
    chunk = vmem((2, WIDE, WIDE), F32)
    whole = [vmem((ND, NF), BF), vmem((ND, NF), BF), vmem((NF, ND), BF)]
    sems = sem((3, WHOLE + 1))
    gate0, up0, act0, h1, a0 = by_tokens(first_kernel, [x], weights, [float(NF), float(NF), NF, ND, ND], [*whole, sems])
    act1, dgate1, dup1, dh1, a1 = by_tokens(second_kernel, [h1, dy], weights, [NF, NF, NF, ND, ND], [*whole, chunk, chunk, chunk, sems])
    return dy, a1, dh1, a0, act1, dgate1, dup1, act0, gate0, up0


RING = [(device_at(p, 0), device_at((p + 1) % 8, 0)) for p in range(8)] + [(device_at(p, 1), device_at((p + 7) % 8, 1)) for p in range(8)]
MATE = [(i, i ^ 1) for i in range(16)]


def solution(mesh):
    def step(x, dy, *state):
        gu, gu_mate, dn, dn_mate, factor, *_ = reduce_call(*front(x[0], dy[0], state[:3]), state[2])
        gu, gu_mate = gu.reshape(2, 2, 64, NF), gu_mate.reshape(2, 2, 64, NF)
        core, rank, *_ = place()
        pos = chip_of(lax.axis_index("dp"))
        other = rank_of(pos, 1 - core)
        new = None
        for s in range(8):
            mine, its = (rank - s) % 8, (other - s) % 8
            where = jnp.stack([8 * core + mine, 8 * (1 - core) + its, rank_of(mine, core), rank_of(its, 1 - core), core, 1 - core]).astype(jnp.int32)
            if s:
                gu = lax.ppermute(gu, "dp", RING)
                dn = lax.ppermute(dn, "dp", RING)
                gu_mate = lax.ppermute(gu, "dp", MATE)
                dn_mate = lax.ppermute(dn, "dp", MATE)
            new = adamw_call(where, factor[:1, :1], (gu, gu_mate, dn, dn_mate), state, new)
        return tuple(new)

    return jax.shard_map(
        step,
        mesh=mesh,
        in_specs=(P(("rep", "dp"), None, None),) * 2 + (P(None, None, None),) * 9,
        out_specs=(P("rep", None, None),) * 9,
        check_vma=False,
    )
```
